32 devices in a mesh: ta: 2 (over x), gz: 4 (over z), xy: 4 (over y, core).
Axes of the slice: x: 2, y: 2, z: 4, core: 2. Of those that a mesh axis runs over, the one named last changes fastest.
Arguments:
- source: float32 [2, 48, 2, 4, 512], P(None, None, 'ta', 'gz', 'xy'), may hold values from -14 to 14
- inverse: bfloat16 [2, 48, 48, 2, 4, 512], P(None, None, None, 'ta', 'gz', 'xy'), may hold values from -0.625 to 0.625
- coarse_links: bfloat16 [8, 2, 48, 48, 2, 4, 512], P(None, None, None, None, 'ta', 'gz', 'xy'), may hold values from -0.15625 to 0.15625
Outputs:
- solution: float32 [2, 48, 2, 4, 512], P(None, None, 'ta', 'gz', 'xy')
- residual: float32 [2, 48, 2, 4, 512], P(None, None, 'ta', 'gz', 'xy')
- hessenberg: float32 [2, 6, 5], replicated
The draws below stay inside these ranges and needn't reach their ends.
All inputs are finite; a program needn't handle non-finite values.
Results may differ from the reference program's by a relative error of at most 0.0003.
Values sent between devices are 32-bit elements; how exact they have to be, the bound alone decides.
A program may use at most 128 MiB of HBM per device.

```python
import jax
import jax.numpy as jnp
from jax import lax

COMP = 48
LY = 16
ITERS = 5
NT = 2
NZ = 4
NXY = 512


def draw_source(key, part):
    key_scale, key_noise = jax.random.split(jax.random.fold_in(key, 11))
    time_pos = jnp.arange(NT).astype(jnp.float32)[:, None, None] / max(NT - 1, 1)
    spread = jax.random.uniform(key_scale, (NT, NZ, NXY), jnp.float32)
    site_scale = 10.0 ** (0.5 * time_pos + 0.5 * spread) / 3.0
    fluctuation = jnp.clip(jax.random.normal(key_noise, (2, COMP, NT, NZ, NXY), jnp.float32), -4.0, 4.0)
    values = fluctuation * site_scale
    return values


def block_levels(own_key, extent, cuts, smallest, top_value):
    loudness = 1.0
    for dim, blocks in cuts:
        draws = jax.random.uniform(jax.random.fold_in(jax.random.fold_in(own_key, 6), dim), (blocks,), jnp.float32, smallest / len(cuts), top_value / len(cuts))
        loudness = loudness * jnp.repeat(jnp.exp(draws), extent[dim] // blocks).reshape((-1,) + (1,) * (len(extent) - 1 - dim))
    return loudness


def scatter_about(rng, shape, width, most, shards=(), dtype=jnp.bfloat16):
    array = jax.random.normal(rng, shape, jnp.float32) * width
    if len(shards) > 0:
        array = block_levels(rng, shape, shards, -0.22, 0.18) * array
    return jnp.clip(array, min=-most, max=most).astype(dtype)


def setup_inputs(seed: int = 0) -> dict:
    key_of = jax.random.split(jax.random.key(seed), 4)
    source = draw_source(jax.random.fold_in(key_of[3], 71), 0)
    inverse = scatter_about(key_of[1], (2, COMP, COMP, NT, NZ, NXY), (2 * COMP) ** -0.5, 0.625, ((3, 2), (4, 4), (5, 4)))
    coarse_links = scatter_about(key_of[2], (8, 2, COMP, COMP, NT, NZ, NXY), (32 * COMP) ** -0.5, 0.15625, ((4, 2), (5, 4), (6, 4)))
    return dict(source=source, inverse=inverse, coarse_links=coarse_links)


def contract(matrix, part):
    return jnp.einsum('ijtzs,jtzs->itzs', matrix, part, precision=lax.Precision.HIGHEST)

def block_apply(blocks, vector):
    widened = blocks.astype(jnp.float32)
    real_part = contract(widened[0], vector[0]) - contract(widened[1], vector[1])
    imag_part = contract(widened[0], vector[1]) + contract(widened[1], vector[0])
    return jnp.stack([real_part, imag_part])

def complex_dot(left, right):
    real_part = jnp.sum(left[0] * right[0] + left[1] * right[1])
    imag_part = jnp.sum(left[0] * right[1] - left[1] * right[0])
    return (real_part, imag_part)

def scaled(coef_real, coef_imag, vector):
    return jnp.stack([coef_real * vector[0] - coef_imag * vector[1], coef_real * vector[1] + coef_imag * vector[0]])

def y_neighbours(field):
    positions = jnp.arange(field.shape[4]) % LY
    is_last = positions == LY - 1
    is_first = positions == 0
    forward = jnp.where(is_last, jnp.roll(field, LY - 1, axis=4), jnp.roll(field, -1, axis=4))
    backward = jnp.where(is_first, jnp.roll(field, 1 - LY, axis=4), jnp.roll(field, 1, axis=4))
    return (forward, backward)

def neighbour_fields(field):
    forward_y, backward_y = y_neighbours(field)
    return [jnp.roll(field, -1, axis=2), jnp.roll(field, 1, axis=2), jnp.roll(field, -1, axis=3), jnp.roll(field, 1, axis=3), jnp.roll(field, -LY, axis=4), jnp.roll(field, LY, axis=4), forward_y, backward_y]

def apply_operator(field, inverse, coarse_links):
    neighbours = neighbour_fields(field)
    hopping = block_apply(coarse_links[0], neighbours[0])
    for d in range(1, 8):
        hopping = hopping + block_apply(coarse_links[d], neighbours[d])
    return field + block_apply(inverse, hopping)

def solve_small(hessenberg, source_norm):
    upper_half = jnp.concatenate([hessenberg[0], -hessenberg[1]], axis=1)
    lower_half = jnp.concatenate([hessenberg[1], hessenberg[0]], axis=1)
    real_form = jnp.concatenate([upper_half, lower_half], axis=0)
    target = jnp.zeros((2 * (ITERS + 1),), jnp.float32).at[0].set(source_norm)
    normal_mat = jnp.dot(real_form.T, real_form, precision=lax.Precision.HIGHEST)
    projected = jnp.dot(real_form.T, target, precision=lax.Precision.HIGHEST)
    factor = jnp.linalg.cholesky(normal_mat)
    forward_vals = []
    for i in range(2 * ITERS):
        partial_sum = projected[i]
        for k in range(i):
            partial_sum = partial_sum - factor[i, k] * forward_vals[k]
        forward_vals.append(partial_sum / factor[i, i])
    solved = [None] * (2 * ITERS)
    for i in reversed(range(2 * ITERS)):
        partial_sum = forward_vals[i]
        for k in range(i + 1, 2 * ITERS):
            partial_sum = partial_sum - factor[k, i] * solved[k]
        solved[i] = partial_sum / factor[i, i]
    coeffs = jnp.stack(solved)
    return (coeffs[:ITERS], coeffs[ITERS:], target)

def reference(source, inverse, coarse_links):
    norm_sq = complex_dot(source, source)[0]
    source_norm = jnp.sqrt(norm_sq)
    krylov_basis = [source / source_norm]
    hessenberg = jnp.zeros((2, ITERS + 1, ITERS), jnp.float32)
    for j in range(ITERS):
        candidate = apply_operator(krylov_basis[j], inverse, coarse_links)
        products = [complex_dot(krylov_basis[i], candidate) for i in range(j + 1)]
        for i in range(j + 1):
            candidate = candidate - scaled(products[i][0], products[i][1], krylov_basis[i])
            hessenberg = hessenberg.at[0, i, j].set(products[i][0]).at[1, i, j].set(products[i][1])
        length = jnp.sqrt(complex_dot(candidate, candidate)[0])
        hessenberg = hessenberg.at[0, j + 1, j].set(length)
        krylov_basis.append(candidate / length)
    coef_real, coef_imag, target = solve_small(hessenberg, source_norm)
    solution = scaled(coef_real[0], coef_imag[0], krylov_basis[0])
    for j in range(1, ITERS):
        solution = solution + scaled(coef_real[j], coef_imag[j], krylov_basis[j])
    residual = source - apply_operator(solution, inverse, coarse_links)
    return (solution, residual, hessenberg)
```

```python
import functools

import jax
import jax.numpy as jnp
from jax import lax
from jax.experimental import pallas as pl
from jax.experimental.pallas import tpu as pltpu
from jax.sharding import PartitionSpec as P

LY = 16
ITERS = 5
SUB = 8
PARTS = 3
DOTS = 2 * ITERS + 1
MESH = pl.DeviceIdType.MESH
ARRIVAL = (6, 7, 4, 5, 0, 1, 2, 3)


def cmul(a, b):
    return (a[0] * b[0] - a[1] * b[1], a[0] * b[1] + a[1] * b[0])


def cmul_conj(a, b):
    return (a[0] * b[0] + a[1] * b[1], a[0] * b[1] - a[1] * b[0])


def cadd(a, b):
    if a is None:
        return b
    return (a[0] + b[0], a[1] + b[1])


def csub(a, b):
    if a is None:
        return (-b[0], -b[1])
    return (a[0] - b[0], a[1] - b[1])


def cscale(a, s):
    return (a[0] * s, a[1] * s)


def conj(a):
    return (a[0], -a[1])


def kernel(sizes, source_hbm, inverse_hbm, links_hbm, sol_ref, res_ref, hes_ref,
           stage, mat_a, mat_b, mat_s, vecs, acc, ys,
           halo_t, halo_z, halo_x, pack, red_one, red_two, red_all, row_one, row_two,
           load_sem, src_sem, t_send, t_recv, z_send, z_recv, x_send, x_recv,
           one_send, one_recv, two_send, two_recv, all_send, all_recv):
    n_ta, n_gz, n_xy = sizes
    comp, lanes = ys.shape[2], ys.shape[3]
    tiles = comp // SUB
    pitch = mat_a.shape[0] // (9 * comp)
    width = comp // PARTS
    me_ta, me_gz, me_xy = (lax.axis_index(a) for a in ("ta", "gz", "xy"))
    n_two = n_ta * n_gz
    n_all = n_two * n_xy
    me_two = me_ta * n_gz + me_gz
    me_all = me_two * n_xy + me_xy
    far = (me_gz + 1) // n_gz

    src = ys.at[0]
    pltpu.make_async_copy(source_hbm, src, src_sem).start()
    loads = []
    for d in ARRIVAL:
        loads.append(pltpu.make_async_copy(links_hbm.at[d], stage.at[d], load_sem.at[d]))
    loads.append(pltpu.make_async_copy(inverse_hbm, stage.at[8], load_sem.at[8]))
    for load in loads:
        load.start()

    def two_peer(k):
        p = lax.rem(me_two + k, n_two)
        return p, {"ta": p // n_gz, "gz": lax.rem(p, n_gz)}

    def all_peer(k):
        p = lax.rem(me_all + k, n_all)
        q = p // n_xy
        return {"ta": q // n_gz, "gz": lax.rem(q, n_gz), "xy": lax.rem(p, n_xy)}

    def step_to(axis, step):
        me, n = {"ta": (me_ta, n_ta), "gz": (me_gz, n_gz), "xy": (me_xy, n_xy)}[axis]
        return {axis: lax.rem(me + step + n, n)}

    barrier = pltpu.get_barrier_semaphore()
    greeted = [all_peer(k) for k in range(1, n_all)]
    for device in greeted:
        pl.semaphore_signal(barrier, inc=1, device_id=device, device_id_type=MESH)
    pltpu.make_async_copy(source_hbm, src, src_sem).wait()
    pl.semaphore_wait(barrier, len(greeted))

    lane = lax.broadcasted_iota(jnp.int32, (SUB, lanes), 1)
    lane_all = lax.broadcasted_iota(jnp.int32, (comp, lanes), 1)
    pending = []

    def remote(s, d, send, recv, device):
        return pltpu.make_async_remote_copy(
            src_ref=s, dst_ref=d, send_sem=send, recv_sem=recv, device_id=device, device_id_type=MESH)

    def go(copy):
        copy.start()
        pending.append(copy)

    def packed(value, first):
        out = jnp.zeros((SUB, lanes), jnp.float32)
        for k in range(tiles):
            tile = value[k * SUB:(k + 1) * SUB]
            shift = (LY * k + (0 if first else LY)) % lanes
            if shift:
                tile = pltpu.roll(tile, shift, 1)
            out = jnp.where(lane // LY == k, tile, out)
        return out

    def unpacked(value, first):
        out = []
        for k in range(tiles):
            shift = ((0 if first else lanes - LY) - LY * k) % lanes
            out.append(pltpu.roll(value, shift, 1) if shift else value)
        return jnp.concatenate(out, axis=0)

    def part(ref, p):
        return ref.at[:, pl.ds(p * width, width)]

    def z_copy(e, slot, p):
        step = 2 * slot - 1
        return remote(part(ys.at[e], p), part(halo_z.at[e, slot], p),
                      z_send.at[e, slot, p], z_recv.at[e, slot, p], step_to("gz", step))

    def t_copy(e, slot):
        return remote(ys.at[e], halo_t.at[e, slot], t_send.at[e, slot], t_recv.at[e, slot],
                      step_to("ta", 2 * slot - 1))

    def x_copy(e, slot):
        return remote(pack.at[e, slot], halo_x.at[e, slot], x_send.at[e, slot], x_recv.at[e, slot],
                      step_to("xy", 2 * slot - 1))

    def send_part(e, p):
        go(z_copy(e, far, p))
        go(z_copy(e, 1 - far, p))

    def send_rest(e):
        for slot in range(1 if n_ta == 2 else 2):
            go(t_copy(e, slot))
        for c in range(2):
            value = ys[e, c]
            pack[e, 0, c] = packed(value, True)
            pack[e, 1, c] = packed(value, False)
        for slot in range(2):
            go(x_copy(e, slot))

    def put(slot, re, im, rows=slice(None)):
        vecs[slot, 0, rows] = re
        vecs[slot, 1, rows] = im - re
        vecs[slot, 2, rows] = re + im

    def set_y(e):
        pos = lane_all % LY
        fwd, bwd = [], []
        for c in range(2):
            v = ys[e, c]
            fwd.append(jnp.where(pos == LY - 1, pltpu.roll(v, LY - 1, 1), pltpu.roll(v, lanes - 1, 1)))
            bwd.append(jnp.where(pos == 0, pltpu.roll(v, lanes - LY + 1, 1), pltpu.roll(v, 1, 1)))
        put(6, *fwd)
        put(7, *bwd)

    def set_x(e):
        fwd, bwd = [], []
        for slot in range(2):
            x_copy(e, slot).wait_recv()
        for c in range(2):
            v = ys[e, c]
            fwd.append(jnp.where(lane_all >= lanes - LY, unpacked(halo_x[e, 0, c], False), pltpu.roll(v, lanes - LY, 1)))
            bwd.append(jnp.where(lane_all < LY, unpacked(halo_x[e, 1, c], True), pltpu.roll(v, LY, 1)))
        put(4, *fwd)
        put(5, *bwd)

    def set_t(e):
        t_copy(e, 0).wait_recv()
        put(0, halo_t[e, 0, 0], halo_t[e, 0, 1])
        back = 0
        if n_ta != 2:
            t_copy(e, 1).wait_recv()
            back = 1
        put(1, halo_t[e, back, 0], halo_t[e, back, 1])

    def set_z(e, slot, vec, p):
        z_copy(e, slot, p).wait_recv()
        rows = pl.ds(p * width, width)
        put(vec, halo_z[e, slot, 0, rows], halo_z[e, slot, 1, rows], rows)

    def convert(d):
        def body(i, _):
            for row in range(2):
                at = i * 2 + row
                a = stage[d, 0, at].astype(jnp.float32)
                b = stage[d, 1, at].astype(jnp.float32)
                s = a + b
                for k in range(tiles):
                    where = pl.ds((d * comp + k * SUB) * pitch + at, SUB, stride=pitch)
                    cols = slice(k * SUB, (k + 1) * SUB)
                    mat_a[where] = a[cols]
                    mat_b[where] = b[cols]
                    mat_s[where] = s[cols]
            return 0

        lax.fori_loop(0, comp // 2, body, 0)

    mats = (mat_s, mat_a, mat_b)

    def sweep(d, vec, first, count, rows, start, unroll=SUB):
        def body(b, sums):
            sums = list(sums)
            for u in range(unroll):
                j = first + b * unroll + u
                base = (d * comp + j) * pitch
                for m in range(3):
                    x = vecs[vec, m, pl.ds(j, SUB, stride=0)]
                    for t, k in enumerate(rows):
                        sums[m * len(rows) + t] += mats[m][pl.ds(base + k * SUB, SUB)] * x
            return tuple(sums)

        return lax.fori_loop(0, count // unroll, body, tuple(start))

    every = range(tiles)

    def products(dirs, first=False):
        if first:
            sums = [jnp.zeros((SUB, lanes), jnp.float32)] * (3 * tiles)
        else:
            sums = [acc[m] for m in range(3 * tiles)]
        for d, vec, begin, count in dirs:
            sums = sweep(d, vec, begin, count, every, sums)
        for m in range(3 * tiles):
            acc[m] = sums[m]

    def whole(d, vec=None):
        return (d, d if vec is None else vec, 0, comp)

    def hop_done():
        for k in every:
            s, a, b = (acc[m * tiles + k] for m in range(3))
            put(8, s - b, s + a, pl.ds(k * SUB, SUB))

    def invert(e, coeffs, then):
        group = tiles // PARTS
        for p in range(PARTS):
            rows = range(p * group, (p + 1) * group)
            sums = sweep(8, 8, 0, comp, rows, [jnp.zeros((SUB, lanes), jnp.float32)] * (3 * group), 2 * SUB)
            for t, k in enumerate(rows):
                s, a, b = (sums[m * group + t] for m in range(3))
                y = (s - b, s + a)
                at = pl.ds(k * SUB, SUB)
                if coeffs is not None:
                    factor, others = coeffs
                    y = cscale(y, factor)
                    for l, u in enumerate(others):
                        if u is not None:
                            y = cadd(y, cmul(u, (ys[l, 0, at], ys[l, 1, at])))
                ys[e + 1, 0, at] = y[0]
                ys[e + 1, 1, at] = y[1]
            then(p)

    row16 = lax.broadcasted_iota(jnp.int32, (2 * SUB, lanes), 0)
    lane16 = lax.broadcasted_iota(jnp.int32, (2 * SUB, lanes), 1)

    def dots(pairs):
        values = []
        for l, i in pairs:
            re = im = None
            for k in every:
                at = pl.ds(k * SUB, SUB)
                r, m = cmul_conj((ys[l, 0, at], ys[l, 1, at]), (ys[i, 0, at], ys[i, 1, at]))
                re = r if re is None else re + r
                im = m if im is None else im + m
            values.append(re)
            if l != i:
                values.append(im)
        table = jnp.zeros((2 * SUB, lanes), jnp.float32)
        for k, value in enumerate(values):
            table = jnp.where(row16 == k, jnp.sum(value, axis=0, keepdims=True), table)
        table = jnp.sum(table, axis=1, keepdims=True)
        return jnp.sum(jnp.where(row16 == lane16, table, 0.0), axis=0, keepdims=True)

    def pairs_of(i):
        return [(l, i) for l in range(i + 1)]

    def start_reduce(j, row):
        row_one[j] = row
        for k in range(1, n_xy):
            go(remote(row_one.at[j], red_one.at[j, me_xy], one_send.at[j, k], one_recv.at[j, me_xy],
                      {"xy": lax.rem(me_xy + k, n_xy)}))
        red_one[j, me_xy] = row

    def middle_reduce(j):
        for k in range(1, n_xy):
            p = lax.rem(me_xy + n_xy - k, n_xy)
            remote(row_one.at[j], red_one.at[j, p], one_send.at[j, k], one_recv.at[j, p], {"xy": p}).wait_recv()
        row = red_one[j, 0]
        for k in range(1, n_xy):
            row = row + red_one[j, k]
        row_two[j] = row
        for k in range(1, n_two):
            go(remote(row_two.at[j], red_two.at[j, me_two], two_send.at[j, k], two_recv.at[j, me_two], two_peer(k)[1]))
        red_two[j, me_two] = row

    def spread(row, count):
        row = jnp.broadcast_to(row, (SUB, lanes))
        return [jnp.broadcast_to(row[:, k:k + 1], (SUB, lanes)) for k in range(count)]

    def end_reduce(j, count):
        for k in range(1, n_two):
            p, device = two_peer(n_two - k)
            remote(row_two.at[j], red_two.at[j, p], two_send.at[j, k], two_recv.at[j, p], device).wait_recv()
        row = red_two[j, 0]
        for k in range(1, n_two):
            row = row + red_two[j, k]
        return spread(row, count)

    last = ITERS - 1

    def all_copy(k):
        return remote(row_one.at[last], red_all.at[me_all], all_send, all_recv, all_peer(k))

    def start_all(row):
        row_one[last] = row
        for k in range(1, n_all):
            all_copy(k).start()
        red_all[me_all] = row

    def end_all(count):
        others = red_all.at[pl.ds(0, n_all - 1)]
        pltpu.make_async_copy(others, others, all_recv).wait()
        terms = [red_all[k] for k in range(n_all)]
        while len(terms) > 1:
            terms = [a + b for a, b in zip(terms[::2], terms[1::2])] + terms[len(terms) & ~1:]
        return spread(terms[0], count)

    n = ITERS + 1
    zero = jnp.zeros((SUB, lanes), jnp.float32)
    one = jnp.ones((SUB, lanes), jnp.float32)
    gram = [[None] * n for _ in range(n)]
    tri = [[None] * n for _ in range(n)]
    inv_tri = [None] * n
    rec = [[None] * ITERS for _ in range(n)]
    shifted = [[None] * ITERS for _ in range(n)]
    hess = [[None] * ITERS for _ in range(n)]

    def set_gram(i, values):
        for l in range(i):
            gram[l][i] = (values[2 * l], values[2 * l + 1])
            gram[i][l] = conj(gram[l][i])
        gram[i][i] = (values[2 * i], zero)
        for l in range(i):
            total = gram[l][i]
            for k in range(l):
                total = csub(total, cmul_conj(tri[k][l], tri[k][i]))
            tri[l][i] = cscale(total, inv_tri[l])
        total = values[2 * i]
        for k in range(i):
            total = total - (tri[k][i][0] * tri[k][i][0] + tri[k][i][1] * tri[k][i][1])
        root = jnp.sqrt(total)
        tri[i][i] = (root, zero)
        inv_tri[i] = 1.0 / root

    def set_rec(i, column):
        for l, value in enumerate(column):
            rec[l][i] = value
            shifted[l][i] = value
        shifted[i][i] = (one if rec[i][i] is None else rec[i][i][0] + 1.0, zero if rec[i][i] is None else rec[i][i][1])

    def next_coeffs(i):
        k = i - 1
        r = [None] * (k + 1)
        r[k] = (inv_tri[k], zero)
        for l in reversed(range(k)):
            total = None
            for m in range(l + 1, k + 1):
                term = cscale(tri[l][m], r[m][0]) if m == k else cmul(tri[l][m], r[m])
                total = csub(total, term)
            r[l] = cscale(total, inv_tri[l])
        t = [None] * (i + 1)
        for m in range(k + 1):
            for l in range(m + 2):
                if rec[l][m] is not None:
                    term = cscale(r[m], rec[l][m][0]) if l == m + 1 else cmul(rec[l][m], r[m])
                    t[l] = cadd(t[l], term)
        u = [None] * (i + 1)
        for m in range(i):
            if t[m] is not None:
                for l in range(m + 2):
                    if rec[l][m] is not None:
                        term = cscale(t[m], rec[l][m][0]) if l == m + 1 else cmul(rec[l][m], t[m])
                        u[l] = cadd(u[l], term)
        factor = t[i][0]
        back = 1.0 / factor
        column = [None if v is None else cscale(v, -back) for v in u] + [(back, zero)]
        set_rec(i, column)
        return factor, u

    def hess_column(j):
        for l in range(j + 2):
            total = None
            for m in range(max(l, 0), j + 2):
                if rec[m][j] is not None:
                    if m == j + 1:
                        term = cscale(tri[l][m], rec[m][j][0])
                    elif m == l:
                        term = cscale(rec[m][j], tri[l][m][0])
                    else:
                        term = cmul(tri[l][m], rec[m][j])
                    total = cadd(total, term)
            for k in range(max(l - 1, 0), j):
                total = csub(total, cmul(hess[l][k], tri[k][j]))
            hess[l][j] = cscale(total, inv_tri[j])

    low = [[None] * ITERS for _ in range(ITERS)]
    inv_low, forward = [], []

    def times(g, b, real):
        return cscale(g, b[0]) if real else cmul(g, b)

    def factor_row(j):
        def g_times(l):
            total = None
            for m in range(j + 2):
                if shifted[m][j] is not None:
                    total = cadd(total, times(gram[l][m], shifted[m][j], m == j + 1))
            return total

        image_j = [g_times(l) for l in range(j + 2)]
        entries = []
        for a in range(j + 1):
            total = None
            for l in range(a + 2):
                if shifted[l][a] is not None:
                    term = cscale(image_j[l], shifted[l][a][0]) if l == a + 1 else cmul_conj(shifted[l][a], image_j[l])
                    total = cadd(total, term)
            entries.append(conj(total))
        for k in range(j):
            total = entries[k]
            for m in range(k):
                total = csub(total, cmul_conj(low[k][m], low[j][m]))
            low[j][k] = cscale(total, inv_low[k])
        diag = entries[j][0]
        for m in range(j):
            diag = diag - (low[j][m][0] * low[j][m][0] + low[j][m][1] * low[j][m][1])
        inv_low.append(1.0 / jnp.sqrt(diag))
        total = None
        for l in range(j + 2):
            if shifted[l][j] is not None:
                term = cscale(gram[l][0], shifted[l][j][0]) if l == j + 1 else cmul_conj(shifted[l][j], gram[l][0])
                total = cadd(total, term)
        for m in range(j):
            total = csub(total, cmul(low[j][m], forward[m]))
        forward.append(cscale(total, inv_low[j]))

    set_rec(0, [None, (one, zero)])
    set_rec(1, [None, None, (one, zero)])
    set_rec(last, [None] * ITERS + [(one, zero)])

    for p in range(PARTS):
        send_part(0, p)
    send_rest(0)
    for e in range(ITERS):
        if e:
            start_reduce(e - 1, dots([(0, 0), (0, 1), (1, 1)] if e == 1 else pairs_of(e)))
            set_y(e)
            products([whole(6), whole(7)], True)
            set_x(e)
            products([whole(4), whole(5)])
            set_t(e)
            products([whole(0), whole(1)])
            middle_reduce(e - 1)
            for p in range(PARTS):
                set_z(e, far, 2, p)
            products([whole(2 + far, 2)])
        else:
            for at, d in enumerate(ARRIVAL[:6]):
                if d == 6:
                    set_y(0)
                elif d == 4:
                    set_x(0)
                elif d == 0:
                    set_t(0)
                loads[at].wait()
                convert(d)
                products([whole(d)], at == 0)
            for at in (6, 7, 8):
                loads[at].wait()
                convert((ARRIVAL + (8,))[at])
            for p in range(PARTS):
                set_z(0, far, 2, p)
            products([whole(2 + far, 2)])
        coeffs = None
        if e == 2:
            values = end_reduce(0, 4)
            set_gram(0, values[:1])
            set_gram(1, values[1:])
            coeffs = next_coeffs(2)
        elif e == 3:
            set_gram(2, end_reduce(1, 5))
            coeffs = next_coeffs(3)
        elif e == 4:
            set_gram(3, end_reduce(2, 7))
        for p in range(PARTS):
            set_z(e, 1 - far, 3, p)
            products([(3 - far, 3, p * width, width)])
        hop_done()
        if e < last:
            invert(e, coeffs, functools.partial(send_part, e + 1))
            send_rest(e + 1)
        else:
            invert(e, coeffs, lambda p: None)
    start_all(dots(pairs_of(ITERS)))

    for j in range(3):
        hess_column(j)
        factor_row(j)
    set_gram(4, end_reduce(3, 9))
    hess_column(3)
    factor_row(3)

    shape = hes_ref.shape[1:]
    part_at = lax.broadcasted_iota(jnp.int32, shape, 0)
    row_at = lax.broadcasted_iota(jnp.int32, shape, 1)

    def write_column(j):
        table = jnp.zeros(shape, jnp.float32)
        for i in range(j + 2):
            re, im = (x[:shape[0], :shape[1]] for x in hess[i][j])
            re = re + 1.0 if i == j else re
            table = jnp.where(row_at == i, jnp.where(part_at == 0, re, im), table)
        hes_ref[j] = table

    for j in range(last):
        write_column(j)

    set_gram(5, end_all(DOTS))
    factor_row(last)
    weights = [None] * ITERS
    for j in reversed(range(ITERS)):
        total = forward[j]
        for m in range(j + 1, ITERS):
            total = csub(total, cmul_conj(low[m][j], weights[m]))
        weights[j] = cscale(total, inv_low[j])
    outer = [None] * n
    for j in range(ITERS):
        for l in range(j + 2):
            if shifted[l][j] is not None:
                outer[l] = cadd(outer[l], times(weights[j], shifted[l][j], l == j + 1))
    for k in every:
        at = pl.ds(k * SUB, SUB)
        left = (ys[0, 0, at], ys[0, 1, at])
        answer = None
        for l in range(n):
            y = (ys[l, 0, at], ys[l, 1, at])
            if l < ITERS:
                answer = cadd(answer, cmul(weights[l], y))
            left = csub(left, cmul(outer[l], y))
        for c in range(2):
            sol_ref[c, at] = answer[c]
            res_ref[c, at] = left[c]
    hess_column(last)
    write_column(last)

    for cp in pending:
        cp.wait_send()
    others = red_all.at[pl.ds(0, n_all - 1)]
    pltpu.make_async_copy(others, others, all_send).wait()


def hand_on(*refs):
    half = len(refs) // 2
    for i in range(half):
        refs[half + i][...] = refs[i][...]


def solution(mesh):
    sizes = tuple(mesh.shape[a] for a in ("ta", "gz", "xy"))

    def per_device(source, inverse, coarse_links):
        comp, lanes = source.shape[1], source.shape[4]
        f32 = jnp.float32
        field = (2, comp, lanes)
        pitch = comp + 1
        mats = (9 * comp * pitch, lanes)
        n_two = sizes[0] * sizes[1]
        dma = pltpu.SemaphoreType.DMA
        hbm = pl.BlockSpec(memory_space=pl.ANY)
        vmem = pl.BlockSpec(memory_space=pltpu.VMEM)
        sol, res, hes = pl.pallas_call(
            functools.partial(kernel, sizes),
            out_shape=(
                jax.ShapeDtypeStruct(field, f32),
                jax.ShapeDtypeStruct(field, f32),
                jax.ShapeDtypeStruct((ITERS, 2, ITERS + 1), f32),
            ),
            in_specs=[hbm, hbm, hbm],
            out_specs=(vmem, vmem, vmem),
            scratch_shapes=[
                pltpu.VMEM((9, 2, comp, comp, lanes), coarse_links.dtype),
                pltpu.VMEM(mats, f32),
                pltpu.VMEM(mats, f32),
                pltpu.VMEM(mats, f32),
                pltpu.VMEM((9, 3, comp, lanes), f32),
                pltpu.VMEM((3 * comp // SUB, SUB, lanes), f32),
                pltpu.VMEM((ITERS + 1, *field), f32),
                pltpu.VMEM((ITERS, 2, *field), f32),
                pltpu.VMEM((ITERS, 2, *field), f32),
                pltpu.VMEM((ITERS, 2, 2, SUB, lanes), f32),
                pltpu.VMEM((ITERS, 2, 2, SUB, lanes), f32),
                pltpu.VMEM((ITERS - 1, sizes[2], 1, lanes), f32),
                pltpu.VMEM((ITERS - 1, n_two, 1, lanes), f32),
                pltpu.VMEM((n_two * sizes[2], 1, lanes), f32),
                pltpu.VMEM((ITERS, 1, lanes), f32),
                pltpu.VMEM((ITERS - 1, 1, lanes), f32),
                dma((9,)),
                dma,
                dma((ITERS, 2)), dma((ITERS, 2)),
                dma((ITERS, 2, PARTS)), dma((ITERS, 2, PARTS)),
                dma((ITERS, 2)), dma((ITERS, 2)),
                dma((ITERS - 1, sizes[2])), dma((ITERS - 1, sizes[2])),
                dma((ITERS - 1, n_two)), dma((ITERS - 1, n_two)),
                dma, dma,
            ],
            compiler_params=pltpu.CompilerParams(
                collective_id=0, has_side_effects=True, vmem_limit_bytes=62 * 1024 * 1024),
        )(
            source.reshape(field),
            inverse.reshape(2, comp, comp, lanes),
            coarse_links.reshape(8, 2, comp, comp, lanes),
        )
        results = (sol, res, hes)
        sol, res, hes = pl.pallas_call(
            hand_on,
            out_shape=tuple(jax.ShapeDtypeStruct(x.shape, x.dtype) for x in results),
            in_specs=[vmem] * 3,
            out_specs=(vmem,) * 3,
        )(*results)
        return sol.reshape(source.shape), res.reshape(source.shape), hes.transpose(1, 2, 0)

    specs = (
        P(None, None, "ta", "gz", "xy"),
        P(None, None, None, "ta", "gz", "xy"),
        P(None, None, None, None, "ta", "gz", "xy"),
    )
    return jax.shard_map(
        per_device,
        mesh=mesh,
        in_specs=specs,
        out_specs=(specs[0], specs[0], P()),
        check_vma=False,
    )
```

```python
import functools

import jax
import jax.numpy as jnp
from jax import lax
from jax.experimental import pallas as pl
from jax.experimental.pallas import tpu as pltpu
from jax.sharding import PartitionSpec as P

LY = 16
ITERS = 5
SUB = 8
PARTS = 3
DOTS = 2 * ITERS + 1
MESH = pl.DeviceIdType.MESH
ARRIVAL = (6, 7, 2, 3, 8, 4, 5, 0, 1)


def cmul(a, b):
    return (a[0] * b[0] - a[1] * b[1], a[0] * b[1] + a[1] * b[0])


def cmul_conj(a, b):
    return (a[0] * b[0] + a[1] * b[1], a[0] * b[1] - a[1] * b[0])


def cadd(a, b):
    if a is None:
        return b
    return (a[0] + b[0], a[1] + b[1])


def csub(a, b):
    if a is None:
        return (-b[0], -b[1])
    return (a[0] - b[0], a[1] - b[1])


def cscale(a, s):
    return (a[0] * s, a[1] * s)


def conj(a):
    return (a[0], -a[1])


def kernel(sizes, source_hbm, inverse_hbm, links_hbm, sol_ref, res_ref, hes_ref,
           stage, mat_a, mat_b, mat_s, vecs, acc, early, ys,
           halo_t, halo_z, halo_x, pack, red_one, red_two, red_all, row_one, row_two,
           load_sem, src_sem, t_send, t_recv, z_send, z_recv, x_send, x_recv,
           one_send, one_recv, two_send, two_recv, all_send, all_recv):
    n_ta, n_gz, n_xy = sizes
    comp, lanes = ys.shape[2], ys.shape[3]
    tiles = comp // SUB
    pitch = mat_a.shape[0] // (9 * comp)
    width = comp // PARTS
    me_ta, me_gz, me_xy = (lax.axis_index(a) for a in ("ta", "gz", "xy"))
    n_two = n_ta * n_gz
    n_all = n_two * n_xy
    me_two = me_ta * n_gz + me_gz
    me_all = me_two * n_xy + me_xy
    far = (me_gz + 1) // n_gz

    src = ys.at[0]
    pltpu.make_async_copy(source_hbm, src, src_sem).start()
    loads = {}
    for d in ARRIVAL:
        block = inverse_hbm if d == 8 else links_hbm.at[d]
        loads[d] = pltpu.make_async_copy(block, stage.at[d], load_sem.at[d])
        loads[d].start()

    def two_peer(k):
        p = lax.rem(me_two + k, n_two)
        return p, {"ta": p // n_gz, "gz": lax.rem(p, n_gz)}

    def all_peer(k):
        p = lax.rem(me_all + k, n_all)
        q = p // n_xy
        return {"ta": q // n_gz, "gz": lax.rem(q, n_gz), "xy": lax.rem(p, n_xy)}

    def step_to(axis, step):
        me, n = {"ta": (me_ta, n_ta), "gz": (me_gz, n_gz), "xy": (me_xy, n_xy)}[axis]
        return {axis: lax.rem(me + step + n, n)}

    barrier = pltpu.get_barrier_semaphore()
    if n_xy // 2 <= 2 and n_ta // 2 + n_gz // 2 <= 3:
        greeted = [step_to(axis, step) for axis, size in (("xy", n_xy), ("gz", n_gz), ("ta", n_ta))
                   for step in ((1, -1) if size > 2 else (1,))]
    else:
        greeted = [all_peer(k) for k in range(1, n_all)]
    for device in greeted:
        pl.semaphore_signal(barrier, inc=1, device_id=device, device_id_type=MESH)
    pltpu.make_async_copy(source_hbm, src, src_sem).wait()
    pl.semaphore_wait(barrier, len(greeted))

    lane = lax.broadcasted_iota(jnp.int32, (SUB, lanes), 1)
    lane_all = lax.broadcasted_iota(jnp.int32, (comp, lanes), 1)
    pending = []

    def remote(s, d, send, recv, device):
        return pltpu.make_async_remote_copy(
            src_ref=s, dst_ref=d, send_sem=send, recv_sem=recv, device_id=device, device_id_type=MESH)

    def go(copy):
        copy.start()
        pending.append(copy)

    def packed(value, first):
        out = jnp.zeros((SUB, lanes), jnp.float32)
        for k in range(tiles):
            tile = value[k * SUB:(k + 1) * SUB]
            shift = (LY * k + (0 if first else LY)) % lanes
            if shift:
                tile = pltpu.roll(tile, shift, 1)
            out = jnp.where(lane // LY == k, tile, out)
        return out

    def unpacked(value, first):
        out = []
        for k in range(tiles):
            shift = ((0 if first else lanes - LY) - LY * k) % lanes
            out.append(pltpu.roll(value, shift, 1) if shift else value)
        return jnp.concatenate(out, axis=0)

    def part(ref, p):
        return ref.at[:, pl.ds(p * width, width)]

    def z_copy(e, slot, p):
        step = 2 * slot - 1
        return remote(part(ys.at[e], p), part(halo_z.at[e, slot], p),
                      z_send.at[e, slot, p], z_recv.at[e, slot, p], step_to("gz", step))

    def t_copy(e, slot):
        return remote(ys.at[e], halo_t.at[e, slot], t_send.at[e, slot], t_recv.at[e, slot],
                      step_to("ta", 2 * slot - 1))

    def x_copy(e, slot):
        return remote(pack.at[e, slot], halo_x.at[e, slot], x_send.at[e, slot], x_recv.at[e, slot],
                      step_to("xy", 2 * slot - 1))

    def send_part(e, p):
        go(z_copy(e, far, p))
        go(z_copy(e, 1 - far, p))

    def send_rest(e):
        for slot in range(1 if n_ta == 2 else 2):
            go(t_copy(e, slot))
        for c in range(2):
            value = ys[e, c]
            pack[e, 0, c] = packed(value, True)
            pack[e, 1, c] = packed(value, False)
        for slot in range(2):
            go(x_copy(e, slot))

    def put(slot, re, im, rows=slice(None)):
        vecs[slot, 0, rows] = re
        vecs[slot, 1, rows] = im - re
        vecs[slot, 2, rows] = re + im

    def set_y(e):
        pos = lane_all % LY
        fwd, bwd = [], []
        for c in range(2):
            v = ys[e, c]
            fwd.append(jnp.where(pos == LY - 1, pltpu.roll(v, LY - 1, 1), pltpu.roll(v, lanes - 1, 1)))
            bwd.append(jnp.where(pos == 0, pltpu.roll(v, lanes - LY + 1, 1), pltpu.roll(v, 1, 1)))
        put(6, *fwd)
        put(7, *bwd)

    def set_x_early(e):
        sides = []
        for c in range(2):
            v = ys[e, c]
            sides.append(jnp.where(lane_all < lanes - LY, pltpu.roll(v, lanes - LY, 1), pltpu.roll(v, LY, 1)))
        put(4, *sides)

    def set_x_late(e):
        for slot in range(2):
            x_copy(e, slot).wait_recv()
        sides = []
        for c in range(2):
            side = jnp.where(lane_all < LY, unpacked(halo_x[e, 1, c], True), pltpu.roll(ys[e, c], LY, 1))
            sides.append(jnp.where(lane_all < lanes - LY, side, unpacked(halo_x[e, 0, c], False)))
        put(5, *sides)

    def set_t(e):
        t_copy(e, 0).wait_recv()
        put(0, halo_t[e, 0, 0], halo_t[e, 0, 1])
        if n_ta != 2:
            t_copy(e, 1).wait_recv()
            put(1, halo_t[e, 1, 0], halo_t[e, 1, 1])

    def set_z(e, slot, vec, p):
        z_copy(e, slot, p).wait_recv()
        rows = pl.ds(p * width, width)
        put(vec, halo_z[e, slot, 0, rows], halo_z[e, slot, 1, rows], rows)

    def keep(d, at, a, b, s):
        for k in range(tiles):
            where = pl.ds((d * comp + k * SUB) * pitch + at, SUB, stride=pitch)
            cols = slice(k * SUB, (k + 1) * SUB)
            mat_a[where] = a[cols]
            mat_b[where] = b[cols]
            mat_s[where] = s[cols]

    def widened(d, at):
        return [stage[d, c, at].astype(jnp.float32) for c in range(2)]

    def convert(d):
        loads[d].wait()

        def body(i, _):
            for u in range(2):
                at = i * 2 + u
                a, b = widened(d, at)
                keep(d, at, a, b, a + b)
            return 0

        lax.fori_loop(0, comp // 2, body, 0)

    def absorb(dirs, mix, first=False):
        for d in dirs:
            loads[d].wait()

        def body(i, _):
            for u in range(2):
                at = i * 2 + u
                sums = [None if first else early[m, at] for m in range(3)]
                for d, (a, b) in mix([widened(d, at) for d in dirs]):
                    s = a + b
                    keep(d, at, a, b, s)
                    for m, x in enumerate((s, a, b)):
                        for k in range(tiles):
                            cols = slice(k * SUB, (k + 1) * SUB)
                            term = x[cols] * vecs[d, m, cols]
                            sums[m] = term if sums[m] is None else sums[m] + term
                for m in range(3):
                    early[m, at] = sums[m]
            return 0

        lax.fori_loop(0, comp // 2, body, 0)

    def plain(*dirs):
        return lambda pairs: list(zip(dirs, pairs))

    def mix_x(pairs):
        low_side = lane_all < lanes - LY
        return [(4, [jnp.where(low_side, f, b) for f, b in zip(*pairs)]),
                (5, [jnp.where(low_side, b, f) for f, b in zip(*pairs)])]

    def mix_t(pairs):
        return [(0, [f + b for f, b in zip(*pairs)])]

    def fold_early():
        for k in range(tiles):
            rows = slice(k * SUB, (k + 1) * SUB)
            s, a, b = (early[m, rows] for m in range(3))
            acc[k] = jnp.zeros((SUB, lanes), jnp.float32)
            acc[tiles + k] = jnp.sum(s + a, axis=1)
            acc[2 * tiles + k] = jnp.sum(b - s, axis=1)

    mats = (mat_s, mat_a, mat_b)

    def sweep(d, vec, first, count, rows, start, unroll=SUB):
        def body(b, sums):
            sums = list(sums)
            for u in range(unroll):
                j = first + b * unroll + u
                base = (d * comp + j) * pitch
                for m in range(3):
                    x = vecs[vec, m, pl.ds(j, SUB, stride=0)]
                    for t, k in enumerate(rows):
                        sums[m * len(rows) + t] += mats[m][pl.ds(base + k * SUB, SUB)] * x
            return tuple(sums)

        return lax.fori_loop(0, count // unroll, body, tuple(start))

    every = range(tiles)

    def products(dirs, first=False):
        if first:
            sums = [jnp.zeros((SUB, lanes), jnp.float32)] * (3 * tiles)
        else:
            sums = [acc[m] for m in range(3 * tiles)]
        for d, vec, begin, count in dirs:
            sums = sweep(d, vec, begin, count, every, sums)
        for m in range(3 * tiles):
            acc[m] = sums[m]

    def whole(d, vec=None):
        return (d, d if vec is None else vec, 0, comp)

    def hop_done():
        for k in every:
            s, a, b = (acc[m * tiles + k] for m in range(3))
            put(8, s - b, s + a, pl.ds(k * SUB, SUB))

    def invert(e, coeffs, then):
        group = tiles // PARTS
        for p in range(PARTS):
            rows = range(p * group, (p + 1) * group)
            sums = sweep(8, 8, 0, comp, rows, [jnp.zeros((SUB, lanes), jnp.float32)] * (3 * group), comp)
            for t, k in enumerate(rows):
                s, a, b = (sums[m * group + t] for m in range(3))
                y = (s - b, s + a)
                at = pl.ds(k * SUB, SUB)
                if coeffs is not None:
                    factor, others = coeffs
                    y = cscale(y, factor)
                    for l, u in enumerate(others):
                        if u is not None:
                            y = cadd(y, cmul(u, (ys[l, 0, at], ys[l, 1, at])))
                ys[e + 1, 0, at] = y[0]
                ys[e + 1, 1, at] = y[1]
            then(p)

    row16 = lax.broadcasted_iota(jnp.int32, (2 * SUB, lanes), 0)
    lane16 = lax.broadcasted_iota(jnp.int32, (2 * SUB, lanes), 1)

    def dots(pairs):
        values = []
        for l, i in pairs:
            re = im = None
            for k in every:
                at = pl.ds(k * SUB, SUB)
                r, m = cmul_conj((ys[l, 0, at], ys[l, 1, at]), (ys[i, 0, at], ys[i, 1, at]))
                re = r if re is None else re + r
                im = m if im is None else im + m
            values.append(re)
            if l != i:
                values.append(im)
        table = jnp.zeros((2 * SUB, lanes), jnp.float32)
        for k, value in enumerate(values):
            table = jnp.where(row16 == k, jnp.sum(value, axis=0, keepdims=True), table)
        table = jnp.sum(table, axis=1, keepdims=True)
        return jnp.sum(jnp.where(row16 == lane16, table, 0.0), axis=0, keepdims=True)

    def pairs_of(i):
        return [(l, i) for l in range(i + 1)]

    def start_reduce(j, row):
        row_one[j] = row
        for k in range(1, n_xy):
            go(remote(row_one.at[j], red_one.at[j, me_xy], one_send.at[j, k], one_recv.at[j, me_xy],
                      {"xy": lax.rem(me_xy + k, n_xy)}))
        red_one[j, me_xy] = row

    def middle_reduce(j):
        for k in range(1, n_xy):
            p = lax.rem(me_xy + n_xy - k, n_xy)
            remote(row_one.at[j], red_one.at[j, p], one_send.at[j, k], one_recv.at[j, p], {"xy": p}).wait_recv()
        row = red_one[j, 0]
        for k in range(1, n_xy):
            row = row + red_one[j, k]
        row_two[j] = row
        for k in range(1, n_two):
            go(remote(row_two.at[j], red_two.at[j, me_two], two_send.at[j, k], two_recv.at[j, me_two], two_peer(k)[1]))
        red_two[j, me_two] = row

    def spread(row, count):
        row = jnp.broadcast_to(row, (SUB, lanes))
        return [jnp.broadcast_to(row[:, k:k + 1], (SUB, lanes)) for k in range(count)]

    def end_reduce(j, count):
        for k in range(1, n_two):
            p, device = two_peer(n_two - k)
            remote(row_two.at[j], red_two.at[j, p], two_send.at[j, k], two_recv.at[j, p], device).wait_recv()
        row = red_two[j, 0]
        for k in range(1, n_two):
            row = row + red_two[j, k]
        return spread(row, count)

    last = ITERS - 1

    def all_copy(k):
        return remote(row_one.at[last], red_all.at[me_all], all_send, all_recv, all_peer(k))

    def start_all(row):
        row_one[last] = row
        for k in range(1, n_all):
            all_copy(k).start()
        red_all[me_all] = row

    def end_all(count):
        others = red_all.at[pl.ds(0, n_all - 1)]
        pltpu.make_async_copy(others, others, all_recv).wait()
        terms = [red_all[k] for k in range(n_all)]
        while len(terms) > 1:
            terms = [a + b for a, b in zip(terms[::2], terms[1::2])] + terms[len(terms) & ~1:]
        return spread(terms[0], count)

    n = ITERS + 1
    zero = jnp.zeros((SUB, lanes), jnp.float32)
    one = jnp.ones((SUB, lanes), jnp.float32)
    gram = [[None] * n for _ in range(n)]
    tri = [[None] * n for _ in range(n)]
    inv_tri = [None] * n
    rec = [[None] * ITERS for _ in range(n)]
    shifted = [[None] * ITERS for _ in range(n)]
    hess = [[None] * ITERS for _ in range(n)]

    def set_gram(i, values):
        for l in range(i):
            gram[l][i] = (values[2 * l], values[2 * l + 1])
            gram[i][l] = conj(gram[l][i])
        gram[i][i] = (values[2 * i], zero)
        for l in range(i):
            total = gram[l][i]
            for k in range(l):
                total = csub(total, cmul_conj(tri[k][l], tri[k][i]))
            tri[l][i] = cscale(total, inv_tri[l])
        total = values[2 * i]
        for k in range(i):
            total = total - (tri[k][i][0] * tri[k][i][0] + tri[k][i][1] * tri[k][i][1])
        root = jnp.sqrt(total)
        tri[i][i] = (root, zero)
        inv_tri[i] = 1.0 / root

    def set_rec(i, column):
        for l, value in enumerate(column):
            rec[l][i] = value
            shifted[l][i] = value
        shifted[i][i] = (one if rec[i][i] is None else rec[i][i][0] + 1.0, zero if rec[i][i] is None else rec[i][i][1])

    def next_coeffs(i):
        k = i - 1
        r = [None] * (k + 1)
        r[k] = (inv_tri[k], zero)
        for l in reversed(range(k)):
            total = None
            for m in range(l + 1, k + 1):
                term = cscale(tri[l][m], r[m][0]) if m == k else cmul(tri[l][m], r[m])
                total = csub(total, term)
            r[l] = cscale(total, inv_tri[l])
        t = [None] * (i + 1)
        for m in range(k + 1):
            for l in range(m + 2):
                if rec[l][m] is not None:
                    term = cscale(r[m], rec[l][m][0]) if l == m + 1 else cmul(rec[l][m], r[m])
                    t[l] = cadd(t[l], term)
        u = [None] * (i + 1)
        for m in range(i):
            if t[m] is not None:
                for l in range(m + 2):
                    if rec[l][m] is not None:
                        term = cscale(t[m], rec[l][m][0]) if l == m + 1 else cmul(rec[l][m], t[m])
                        u[l] = cadd(u[l], term)
        factor = t[i][0]
        back = 1.0 / factor
        column = [None if v is None else cscale(v, -back) for v in u] + [(back, zero)]
        set_rec(i, column)
        return factor, u

    def hess_column(j):
        for l in range(j + 2):
            total = None
            for m in range(max(l, 0), j + 2):
                if rec[m][j] is not None:
                    if m == j + 1:
                        term = cscale(tri[l][m], rec[m][j][0])
                    elif m == l:
                        term = cscale(rec[m][j], tri[l][m][0])
                    else:
                        term = cmul(tri[l][m], rec[m][j])
                    total = cadd(total, term)
            for k in range(max(l - 1, 0), j):
                total = csub(total, cmul(hess[l][k], tri[k][j]))
            hess[l][j] = cscale(total, inv_tri[j])

    low = [[None] * ITERS for _ in range(ITERS)]
    inv_low, forward = [], []

    def times(g, b, real):
        return cscale(g, b[0]) if real else cmul(g, b)

    def factor_row(j):
        def g_times(l):
            total = None
            for m in range(j + 2):
                if shifted[m][j] is not None:
                    total = cadd(total, times(gram[l][m], shifted[m][j], m == j + 1))
            return total

        image_j = [g_times(l) for l in range(j + 2)]
        entries = []
        for a in range(j + 1):
            total = None
            for l in range(a + 2):
                if shifted[l][a] is not None:
                    term = cscale(image_j[l], shifted[l][a][0]) if l == a + 1 else cmul_conj(shifted[l][a], image_j[l])
                    total = cadd(total, term)
            entries.append(conj(total))
        for k in range(j):
            total = entries[k]
            for m in range(k):
                total = csub(total, cmul_conj(low[k][m], low[j][m]))
            low[j][k] = cscale(total, inv_low[k])
        diag = entries[j][0]
        for m in range(j):
            diag = diag - (low[j][m][0] * low[j][m][0] + low[j][m][1] * low[j][m][1])
        inv_low.append(1.0 / jnp.sqrt(diag))
        total = None
        for l in range(j + 2):
            if shifted[l][j] is not None:
                term = cscale(gram[l][0], shifted[l][j][0]) if l == j + 1 else cmul_conj(shifted[l][j], gram[l][0])
                total = cadd(total, term)
        for m in range(j):
            total = csub(total, cmul(low[j][m], forward[m]))
        forward.append(cscale(total, inv_low[j]))

    set_rec(0, [None, (one, zero)])
    set_rec(1, [None, None, (one, zero)])
    set_rec(last, [None] * ITERS + [(one, zero)])

    for p in range(PARTS):
        send_part(0, p)
    send_rest(0)
    t_dirs = (0,) if n_ta == 2 else (0, 1)
    for e in range(ITERS):
        if e:
            start_reduce(e - 1, dots([(0, 0), (0, 1), (1, 1)] if e == 1 else pairs_of(e)))
            set_y(e)
            set_x_early(e)
            products([whole(6), whole(7), whole(4)], True)
            if e > 1:
                middle_reduce(e - 1)
            set_x_late(e)
            products([whole(5)])
            set_t(e)
            products([whole(d) for d in t_dirs])
            if e == 1:
                middle_reduce(0)
        else:
            set_y(0)
            set_x_early(0)
            absorb((6,), plain(6), True)
            absorb((7,), plain(7))
            for d in (2, 3, 8):
                convert(d)
            set_x_late(0)
            absorb((4, 5), mix_x)
            set_t(0)
            absorb((0, 1), mix_t if n_ta == 2 else plain(0, 1))
            fold_early()
        for p in range(PARTS):
            set_z(e, far, 2, p)
        products([whole(2 + far, 2)])
        coeffs = None
        if e == 2:
            values = end_reduce(0, 4)
            set_gram(0, values[:1])
            set_gram(1, values[1:])
            coeffs = next_coeffs(2)
        elif e == 3:
            set_gram(2, end_reduce(1, 5))
            coeffs = next_coeffs(3)
        elif e == 4:
            set_gram(3, end_reduce(2, 7))
        for p in range(PARTS):
            set_z(e, 1 - far, 3, p)
            products([(3 - far, 3, p * width, width)])
        hop_done()
        if e < last:
            invert(e, coeffs, functools.partial(send_part, e + 1))
            send_rest(e + 1)
        else:
            invert(e, coeffs, lambda p: None)
    start_all(dots(pairs_of(ITERS)))

    for j in range(3):
        hess_column(j)
        factor_row(j)
    set_gram(4, end_reduce(3, 9))
    hess_column(3)
    factor_row(3)

    shape = hes_ref.shape[1:]
    part_at = lax.broadcasted_iota(jnp.int32, shape, 0)
    row_at = lax.broadcasted_iota(jnp.int32, shape, 1)

    def write_column(j):
        table = jnp.zeros(shape, jnp.float32)
        for i in range(j + 2):
            re, im = (x[:shape[0], :shape[1]] for x in hess[i][j])
            re = re + 1.0 if i == j else re
            table = jnp.where(row_at == i, jnp.where(part_at == 0, re, im), table)
        hes_ref[j] = table

    for j in range(last):
        write_column(j)

    set_gram(5, end_all(DOTS))
    factor_row(last)
    weights = [None] * ITERS
    for j in reversed(range(ITERS)):
        total = forward[j]
        for m in range(j + 1, ITERS):
            total = csub(total, cmul_conj(low[m][j], weights[m]))
        weights[j] = cscale(total, inv_low[j])
    outer = [None] * n
    for j in range(ITERS):
        for l in range(j + 2):
            if shifted[l][j] is not None:
                outer[l] = cadd(outer[l], times(weights[j], shifted[l][j], l == j + 1))
    for k in every:
        at = pl.ds(k * SUB, SUB)
        left = (ys[0, 0, at], ys[0, 1, at])
        answer = None
        for l in range(n):
            y = (ys[l, 0, at], ys[l, 1, at])
            if l < ITERS:
                answer = cadd(answer, cmul(weights[l], y))
            left = csub(left, cmul(outer[l], y))
        for c in range(2):
            sol_ref[c, at] = answer[c]
            res_ref[c, at] = left[c]
    hess_column(last)
    write_column(last)

    for cp in pending:
        cp.wait_send()
    others = red_all.at[pl.ds(0, n_all - 1)]
    pltpu.make_async_copy(others, others, all_send).wait()


def hand_on(*refs):
    half = len(refs) // 2
    for i in range(half):
        refs[half + i][...] = refs[i][...]


def solution(mesh):
    sizes = tuple(mesh.shape[a] for a in ("ta", "gz", "xy"))

    def per_device(source, inverse, coarse_links):
        comp, lanes = source.shape[1], source.shape[4]
        f32 = jnp.float32
        field = (2, comp, lanes)
        pitch = comp + 1
        mats = (9 * comp * pitch, lanes)
        n_two = sizes[0] * sizes[1]
        dma = pltpu.SemaphoreType.DMA
        hbm = pl.BlockSpec(memory_space=pl.ANY)
        vmem = pl.BlockSpec(memory_space=pltpu.VMEM)
        sol, res, hes = pl.pallas_call(
            functools.partial(kernel, sizes),
            out_shape=(
                jax.ShapeDtypeStruct(field, f32),
                jax.ShapeDtypeStruct(field, f32),
                jax.ShapeDtypeStruct((ITERS, 2, ITERS + 1), f32),
            ),
            in_specs=[hbm, hbm, hbm],
            out_specs=(vmem, vmem, vmem),
            scratch_shapes=[
                pltpu.VMEM((9, 2, comp, comp, lanes), coarse_links.dtype),
                pltpu.VMEM(mats, f32),
                pltpu.VMEM(mats, f32),
                pltpu.VMEM(mats, f32),
                pltpu.VMEM((9, 3, comp, lanes), f32),
                pltpu.VMEM((3 * comp // SUB, SUB, lanes), f32),
                pltpu.VMEM((3, comp, SUB, lanes), f32),
                pltpu.VMEM((ITERS + 1, *field), f32),
                pltpu.VMEM((ITERS, 2, *field), f32),
                pltpu.VMEM((ITERS, 2, *field), f32),
                pltpu.VMEM((ITERS, 2, 2, SUB, lanes), f32),
                pltpu.VMEM((ITERS, 2, 2, SUB, lanes), f32),
                pltpu.VMEM((ITERS - 1, sizes[2], 1, lanes), f32),
                pltpu.VMEM((ITERS - 1, n_two, 1, lanes), f32),
                pltpu.VMEM((n_two * sizes[2], 1, lanes), f32),
                pltpu.VMEM((ITERS, 1, lanes), f32),
                pltpu.VMEM((ITERS - 1, 1, lanes), f32),
                dma((9,)),
                dma,
                dma((ITERS, 2)), dma((ITERS, 2)),
                dma((ITERS, 2, PARTS)), dma((ITERS, 2, PARTS)),
                dma((ITERS, 2)), dma((ITERS, 2)),
                dma((ITERS - 1, sizes[2])), dma((ITERS - 1, sizes[2])),
                dma((ITERS - 1, n_two)), dma((ITERS - 1, n_two)),
                dma, dma,
            ],
            compiler_params=pltpu.CompilerParams(
                collective_id=0, has_side_effects=True, vmem_limit_bytes=62 * 1024 * 1024),
        )(
            source.reshape(field),
            inverse.reshape(2, comp, comp, lanes),
            coarse_links.reshape(8, 2, comp, comp, lanes),
        )
        results = (sol, res, hes)
        sol, res, hes = pl.pallas_call(
            hand_on,
            out_shape=tuple(jax.ShapeDtypeStruct(x.shape, x.dtype) for x in results),
            in_specs=[vmem] * 3,
            out_specs=(vmem,) * 3,
        )(*results)
        return sol.reshape(source.shape), res.reshape(source.shape), hes.transpose(1, 2, 0)

    specs = (
        P(None, None, "ta", "gz", "xy"),
        P(None, None, None, "ta", "gz", "xy"),
        P(None, None, None, None, "ta", "gz", "xy"),
    )
    return jax.shard_map(
        per_device,
        mesh=mesh,
        in_specs=specs,
        out_specs=(specs[0], specs[0], P()),
        check_vma=False,
    )
```

```python
import functools

import jax
import jax.numpy as jnp
from jax import lax
from jax.experimental import pallas as pl
from jax.experimental.pallas import tpu as pltpu
from jax.sharding import PartitionSpec as P

LY = 16
ITERS = 5
SUB = 8
PARTS = 3
DOTS = 2 * ITERS + 1
MESH = pl.DeviceIdType.MESH
ARRIVAL = (6, 7, 2, 3, 8, 4, 5, 0, 1)


def cmul(a, b):
    return (a[0] * b[0] - a[1] * b[1], a[0] * b[1] + a[1] * b[0])


def cmul_conj(a, b):
    return (a[0] * b[0] + a[1] * b[1], a[0] * b[1] - a[1] * b[0])


def cadd(a, b):
    if a is None:
        return b
    return (a[0] + b[0], a[1] + b[1])


def csub(a, b):
    if a is None:
        return (-b[0], -b[1])
    return (a[0] - b[0], a[1] - b[1])


def cscale(a, s):
    return (a[0] * s, a[1] * s)


def conj(a):
    return (a[0], -a[1])


def kernel(sizes, source_hbm, inverse_hbm, links_hbm, sol_ref, res_ref, hes_ref,
           stage, mat_a, mat_b, mat_s, vecs, acc, early, ys,
           halo_t, halo_z, halo_x, pack, red_one, red_two, red_all, row_one, row_two,
           load_sem, src_sem, t_send, t_recv, z_send, z_recv, x_send, x_recv,
           one_send, one_recv, two_send, two_recv, all_send, all_recv):
    n_ta, n_gz, n_xy = sizes
    comp, lanes = ys.shape[2], ys.shape[3]
    tiles = comp // SUB
    pitch = mat_a.shape[0] // (9 * comp)
    width = comp // PARTS
    me_ta, me_gz, me_xy = (lax.axis_index(a) for a in ("ta", "gz", "xy"))
    n_two = n_ta * n_gz
    n_all = n_two * n_xy
    me_two = me_ta * n_gz + me_gz
    me_all = me_two * n_xy + me_xy
    far = (me_gz + 1) // n_gz

    src = ys.at[0]
    pltpu.make_async_copy(source_hbm, src, src_sem).start()
    loads = {}
    for d in ARRIVAL:
        block = inverse_hbm if d == 8 else links_hbm.at[d]
        loads[d] = pltpu.make_async_copy(block, stage.at[d], load_sem.at[d])
        loads[d].start()

    def two_peer(k):
        p = lax.rem(me_two + k, n_two)
        return p, {"ta": p // n_gz, "gz": lax.rem(p, n_gz)}

    def all_peer(k):
        p = lax.rem(me_all + k, n_all)
        q = p // n_xy
        return {"ta": q // n_gz, "gz": lax.rem(q, n_gz), "xy": lax.rem(p, n_xy)}

    def step_to(axis, step):
        me, n = {"ta": (me_ta, n_ta), "gz": (me_gz, n_gz), "xy": (me_xy, n_xy)}[axis]
        return {axis: lax.rem(me + step + n, n)}

    barrier = pltpu.get_barrier_semaphore()
    if n_xy // 2 <= 2 and n_ta // 2 + n_gz // 2 <= 3:
        greeted = [step_to(axis, step) for axis, size in (("xy", n_xy), ("gz", n_gz), ("ta", n_ta))
                   for step in ((1, -1) if size > 2 else (1,))]
    else:
        greeted = [all_peer(k) for k in range(1, n_all)]
    for device in greeted:
        pl.semaphore_signal(barrier, inc=1, device_id=device, device_id_type=MESH)
    pltpu.make_async_copy(source_hbm, src, src_sem).wait()
    pl.semaphore_wait(barrier, len(greeted))

    lane = lax.broadcasted_iota(jnp.int32, (SUB, lanes), 1)
    lane_all = lax.broadcasted_iota(jnp.int32, (comp, lanes), 1)
    pending = []

    def remote(s, d, send, recv, device):
        return pltpu.make_async_remote_copy(
            src_ref=s, dst_ref=d, send_sem=send, recv_sem=recv, device_id=device, device_id_type=MESH)

    def go(copy):
        copy.start()
        pending.append(copy)

    def packed(value, first):
        out = jnp.zeros((SUB, lanes), jnp.float32)
        for k in range(tiles):
            tile = value[k * SUB:(k + 1) * SUB]
            shift = (LY * k + (0 if first else LY)) % lanes
            if shift:
                tile = pltpu.roll(tile, shift, 1)
            out = jnp.where(lane // LY == k, tile, out)
        return out

    def unpacked(value, first):
        out = []
        for k in range(tiles):
            shift = ((0 if first else lanes - LY) - LY * k) % lanes
            out.append(pltpu.roll(value, shift, 1) if shift else value)
        return jnp.concatenate(out, axis=0)

    def part(ref, p):
        return ref.at[:, pl.ds(p * width, width)]

    def z_copy(e, slot, p):
        step = 2 * slot - 1
        return remote(part(ys.at[e], p), part(halo_z.at[e, slot], p),
                      z_send.at[e, slot, p], z_recv.at[e, slot, p], step_to("gz", step))

    def t_copy(e, slot):
        return remote(ys.at[e], halo_t.at[e, slot], t_send.at[e, slot], t_recv.at[e, slot],
                      step_to("ta", 2 * slot - 1))

    def x_copy(e, slot):
        return remote(pack.at[e, slot], halo_x.at[e, slot], x_send.at[e, slot], x_recv.at[e, slot],
                      step_to("xy", 2 * slot - 1))

    def send_part(e, p):
        go(z_copy(e, far, p))
        go(z_copy(e, 1 - far, p))

    def send_rest(e):
        for slot in range(1 if n_ta == 2 else 2):
            go(t_copy(e, slot))
        for c in range(2):
            value = ys[e, c]
            pack[e, 0, c] = packed(value, True)
            pack[e, 1, c] = packed(value, False)
        for slot in range(2):
            go(x_copy(e, slot))

    def put(slot, re, im, rows=slice(None)):
        vecs[slot, 0, rows] = re
        vecs[slot, 1, rows] = im - re
        vecs[slot, 2, rows] = re + im

    def set_y(e):
        pos = lane_all % LY
        fwd, bwd = [], []
        for c in range(2):
            v = ys[e, c]
            fwd.append(jnp.where(pos == LY - 1, pltpu.roll(v, LY - 1, 1), pltpu.roll(v, lanes - 1, 1)))
            bwd.append(jnp.where(pos == 0, pltpu.roll(v, lanes - LY + 1, 1), pltpu.roll(v, 1, 1)))
        put(6, *fwd)
        put(7, *bwd)

    def set_x_early(e):
        sides = []
        for c in range(2):
            v = ys[e, c]
            sides.append(jnp.where(lane_all < lanes - LY, pltpu.roll(v, lanes - LY, 1), pltpu.roll(v, LY, 1)))
        put(4, *sides)

    def set_x_late(e):
        for slot in range(2):
            x_copy(e, slot).wait_recv()
        sides = []
        for c in range(2):
            side = jnp.where(lane_all < LY, unpacked(halo_x[e, 1, c], True), pltpu.roll(ys[e, c], LY, 1))
            sides.append(jnp.where(lane_all < lanes - LY, side, unpacked(halo_x[e, 0, c], False)))
        put(5, *sides)

    def set_t(e):
        t_copy(e, 0).wait_recv()
        put(0, halo_t[e, 0, 0], halo_t[e, 0, 1])
        if n_ta != 2:
            t_copy(e, 1).wait_recv()
            put(1, halo_t[e, 1, 0], halo_t[e, 1, 1])

    def set_z(e, slot, vec, p):
        z_copy(e, slot, p).wait_recv()
        rows = pl.ds(p * width, width)
        put(vec, halo_z[e, slot, 0, rows], halo_z[e, slot, 1, rows], rows)

    def total_of(terms):
        while len(terms) > 1:
            terms = [a + b for a, b in zip(terms[::2], terms[1::2])] + terms[len(terms) & ~1:]
        return terms[0]

    def keep(d, at, a, b, s):
        for k in range(tiles):
            where = pl.ds((d * comp + k * SUB) * pitch + at, SUB, stride=pitch)
            cols = slice(k * SUB, (k + 1) * SUB)
            mat_a[where] = a[cols]
            mat_b[where] = b[cols]
            mat_s[where] = s[cols]

    def widened(d, at):
        return [stage[d, c, at].astype(jnp.float32) for c in range(2)]

    def convert(d):
        loads[d].wait()

        def body(i, _):
            for u in range(2):
                at = i * 2 + u
                a, b = widened(d, at)
                keep(d, at, a, b, a + b)
            return 0

        lax.fori_loop(0, comp // 2, body, 0)

    def absorb(dirs, mix, first=False):
        for d in dirs:
            loads[d].wait()

        def body(i, _):
            for u in range(SUB):
                at = i * SUB + u
                terms = [[] if first else [early[m, at]] for m in range(3)]
                for d, (a, b) in mix([widened(d, at) for d in dirs]):
                    s = a + b
                    keep(d, at, a, b, s)
                    for m, x in enumerate((s, a, b)):
                        for k in range(tiles):
                            cols = slice(k * SUB, (k + 1) * SUB)
                            terms[m].append(x[cols] * vecs[d, m, cols])
                for m in range(3):
                    early[m, at] = total_of(terms[m])
            return 0

        lax.fori_loop(0, comp // SUB, body, 0)

    def plain(*dirs):
        return lambda pairs: list(zip(dirs, pairs))

    def mix_x(pairs):
        low_side = lane_all < lanes - LY
        return [(4, [jnp.where(low_side, f, b) for f, b in zip(*pairs)]),
                (5, [jnp.where(low_side, b, f) for f, b in zip(*pairs)])]

    def mix_t(pairs):
        return [(0, [f + b for f, b in zip(*pairs)])]

    def fold_early():
        for k in range(tiles):
            rows = slice(k * SUB, (k + 1) * SUB)
            s, a, b = (early[m, rows] for m in range(3))
            acc[k] = jnp.zeros((SUB, lanes), jnp.float32)
            acc[tiles + k] = jnp.sum(s + a, axis=1)
            acc[2 * tiles + k] = jnp.sum(b - s, axis=1)

    mats = (mat_s, mat_a, mat_b)

    def sweep(d, vec, first, count, rows, start, unroll=SUB):
        def body(b, sums):
            sums = list(sums)
            for u in range(unroll):
                j = first + b * unroll + u
                base = (d * comp + j) * pitch
                for m in range(3):
                    x = vecs[vec, m, pl.ds(j, SUB, stride=0)]
                    for t, k in enumerate(rows):
                        sums[m * len(rows) + t] += mats[m][pl.ds(base + k * SUB, SUB)] * x
            return tuple(sums)

        return lax.fori_loop(0, count // unroll, body, tuple(start))

    every = range(tiles)

    def products(dirs, first=False):
        if first:
            sums = [jnp.zeros((SUB, lanes), jnp.float32)] * (3 * tiles)
        else:
            sums = [acc[m] for m in range(3 * tiles)]
        for d, vec, begin, count in dirs:
            sums = sweep(d, vec, begin, count, every, sums)
        for m in range(3 * tiles):
            acc[m] = sums[m]

    def whole(d, vec=None):
        return (d, d if vec is None else vec, 0, comp)

    def hop_done():
        for k in every:
            s, a, b = (acc[m * tiles + k] for m in range(3))
            put(8, s - b, s + a, pl.ds(k * SUB, SUB))

    def invert(e, coeffs, then):
        group = tiles // PARTS
        for p in range(PARTS):
            rows = range(p * group, (p + 1) * group)
            sums = sweep(8, 8, 0, comp, rows, [jnp.zeros((SUB, lanes), jnp.float32)] * (3 * group), comp)
            for t, k in enumerate(rows):
                s, a, b = (sums[m * group + t] for m in range(3))
                y = (s - b, s + a)
                at = pl.ds(k * SUB, SUB)
                if coeffs is not None:
                    factor, others = coeffs
                    y = cscale(y, factor)
                    for l, u in enumerate(others):
                        if u is not None:
                            y = cadd(y, cmul(u, (ys[l, 0, at], ys[l, 1, at])))
                ys[e + 1, 0, at] = y[0]
                ys[e + 1, 1, at] = y[1]
            then(p)

    row16 = lax.broadcasted_iota(jnp.int32, (2 * SUB, lanes), 0)
    lane16 = lax.broadcasted_iota(jnp.int32, (2 * SUB, lanes), 1)

    def dots(pairs):
        values = []
        for l, i in pairs:
            re = im = None
            for k in every:
                at = pl.ds(k * SUB, SUB)
                r, m = cmul_conj((ys[l, 0, at], ys[l, 1, at]), (ys[i, 0, at], ys[i, 1, at]))
                re = r if re is None else re + r
                im = m if im is None else im + m
            values.append(re)
            if l != i:
                values.append(im)
        table = jnp.zeros((2 * SUB, lanes), jnp.float32)
        for k, value in enumerate(values):
            table = jnp.where(row16 == k, jnp.sum(value, axis=0, keepdims=True), table)
        table = jnp.sum(table, axis=1, keepdims=True)
        return jnp.sum(jnp.where(row16 == lane16, table, 0.0), axis=0, keepdims=True)

    def pairs_of(i):
        return [(l, i) for l in range(i + 1)]

    def start_reduce(j, row):
        row_one[j] = row
        for k in range(1, n_xy):
            go(remote(row_one.at[j], red_one.at[j, me_xy], one_send.at[j, k], one_recv.at[j, me_xy],
                      {"xy": lax.rem(me_xy + k, n_xy)}))
        red_one[j, me_xy] = row

    def middle_reduce(j):
        for k in range(1, n_xy):
            p = lax.rem(me_xy + n_xy - k, n_xy)
            remote(row_one.at[j], red_one.at[j, p], one_send.at[j, k], one_recv.at[j, p], {"xy": p}).wait_recv()
        row = red_one[j, 0]
        for k in range(1, n_xy):
            row = row + red_one[j, k]
        row_two[j] = row
        for k in range(1, n_two):
            go(remote(row_two.at[j], red_two.at[j, me_two], two_send.at[j, k], two_recv.at[j, me_two], two_peer(k)[1]))
        red_two[j, me_two] = row

    def spread(row, count):
        row = jnp.broadcast_to(row, (SUB, lanes))
        return [jnp.broadcast_to(row[:, k:k + 1], (SUB, lanes)) for k in range(count)]

    def end_reduce(j, count):
        for k in range(1, n_two):
            p, device = two_peer(n_two - k)
            remote(row_two.at[j], red_two.at[j, p], two_send.at[j, k], two_recv.at[j, p], device).wait_recv()
        row = red_two[j, 0]
        for k in range(1, n_two):
            row = row + red_two[j, k]
        return spread(row, count)

    last = ITERS - 1

    def all_copy(k):
        return remote(row_one.at[last], red_all.at[me_all], all_send, all_recv, all_peer(k))

    def start_all(row):
        row_one[last] = row
        for k in range(1, n_all):
            all_copy(k).start()
        red_all[me_all] = row

    def end_all(count):
        others = red_all.at[pl.ds(0, n_all - 1)]
        pltpu.make_async_copy(others, others, all_recv).wait()
        terms = [red_all[k] for k in range(n_all)]
        while len(terms) > 1:
            terms = [a + b for a, b in zip(terms[::2], terms[1::2])] + terms[len(terms) & ~1:]
        return spread(terms[0], count)

    n = ITERS + 1
    zero = jnp.zeros((SUB, lanes), jnp.float32)
    one = jnp.ones((SUB, lanes), jnp.float32)
    gram = [[None] * n for _ in range(n)]
    tri = [[None] * n for _ in range(n)]
    inv_tri = [None] * n
    rec = [[None] * ITERS for _ in range(n)]
    shifted = [[None] * ITERS for _ in range(n)]
    hess = [[None] * ITERS for _ in range(n)]

    def set_gram(i, values):
        for l in range(i):
            gram[l][i] = (values[2 * l], values[2 * l + 1])
            gram[i][l] = conj(gram[l][i])
        gram[i][i] = (values[2 * i], zero)
        for l in range(i):
            total = gram[l][i]
            for k in range(l):
                total = csub(total, cmul_conj(tri[k][l], tri[k][i]))
            tri[l][i] = cscale(total, inv_tri[l])
        total = values[2 * i]
        for k in range(i):
            total = total - (tri[k][i][0] * tri[k][i][0] + tri[k][i][1] * tri[k][i][1])
        root = jnp.sqrt(total)
        tri[i][i] = (root, zero)
        inv_tri[i] = 1.0 / root

    def set_rec(i, column):
        for l, value in enumerate(column):
            rec[l][i] = value
            shifted[l][i] = value
        shifted[i][i] = (one if rec[i][i] is None else rec[i][i][0] + 1.0, zero if rec[i][i] is None else rec[i][i][1])

    def next_coeffs(i):
        k = i - 1
        r = [None] * (k + 1)
        r[k] = (inv_tri[k], zero)
        for l in reversed(range(k)):
            total = None
            for m in range(l + 1, k + 1):
                term = cscale(tri[l][m], r[m][0]) if m == k else cmul(tri[l][m], r[m])
                total = csub(total, term)
            r[l] = cscale(total, inv_tri[l])
        t = [None] * (i + 1)
        for m in range(k + 1):
            for l in range(m + 2):
                if rec[l][m] is not None:
                    term = cscale(r[m], rec[l][m][0]) if l == m + 1 else cmul(rec[l][m], r[m])
                    t[l] = cadd(t[l], term)
        u = [None] * (i + 1)
        for m in range(i):
            if t[m] is not None:
                for l in range(m + 2):
                    if rec[l][m] is not None:
                        term = cscale(t[m], rec[l][m][0]) if l == m + 1 else cmul(rec[l][m], t[m])
                        u[l] = cadd(u[l], term)
        factor = t[i][0]
        back = 1.0 / factor
        column = [None if v is None else cscale(v, -back) for v in u] + [(back, zero)]
        set_rec(i, column)
        return factor, u

    def hess_column(j):
        for l in range(j + 2):
            total = None
            for m in range(max(l, 0), j + 2):
                if rec[m][j] is not None:
                    if m == j + 1:
                        term = cscale(tri[l][m], rec[m][j][0])
                    elif m == l:
                        term = cscale(rec[m][j], tri[l][m][0])
                    else:
                        term = cmul(tri[l][m], rec[m][j])
                    total = cadd(total, term)
            for k in range(max(l - 1, 0), j):
                total = csub(total, cmul(hess[l][k], tri[k][j]))
            hess[l][j] = cscale(total, inv_tri[j])

    low = [[None] * ITERS for _ in range(ITERS)]
    inv_low, forward = [], []

    def times(g, b, real):
        return cscale(g, b[0]) if real else cmul(g, b)

    def factor_row(j):
        def g_times(l):
            total = None
            for m in range(j + 2):
                if shifted[m][j] is not None:
                    total = cadd(total, times(gram[l][m], shifted[m][j], m == j + 1))
            return total

        image_j = [g_times(l) for l in range(j + 2)]
        entries = []
        for a in range(j + 1):
            total = None
            for l in range(a + 2):
                if shifted[l][a] is not None:
                    term = cscale(image_j[l], shifted[l][a][0]) if l == a + 1 else cmul_conj(shifted[l][a], image_j[l])
                    total = cadd(total, term)
            entries.append(conj(total))
        for k in range(j):
            total = entries[k]
            for m in range(k):
                total = csub(total, cmul_conj(low[k][m], low[j][m]))
            low[j][k] = cscale(total, inv_low[k])
        diag = entries[j][0]
        for m in range(j):
            diag = diag - (low[j][m][0] * low[j][m][0] + low[j][m][1] * low[j][m][1])
        inv_low.append(1.0 / jnp.sqrt(diag))
        total = None
        for l in range(j + 2):
            if shifted[l][j] is not None:
                term = cscale(gram[l][0], shifted[l][j][0]) if l == j + 1 else cmul_conj(shifted[l][j], gram[l][0])
                total = cadd(total, term)
        for m in range(j):
            total = csub(total, cmul(low[j][m], forward[m]))
        forward.append(cscale(total, inv_low[j]))

    set_rec(0, [None, (one, zero)])
    set_rec(1, [None, None, (one, zero)])
    set_rec(last, [None] * ITERS + [(one, zero)])

    for p in range(PARTS):
        send_part(0, p)
    send_rest(0)
    t_dirs = (0,) if n_ta == 2 else (0, 1)
    for e in range(ITERS):
        if e:
            start_reduce(e - 1, dots([(0, 0), (0, 1), (1, 1)] if e == 1 else pairs_of(e)))
            set_y(e)
            set_x_early(e)
            products([whole(6), whole(7), whole(4)], True)
            if e > 1:
                middle_reduce(e - 1)
            set_x_late(e)
            products([whole(5)])
            set_t(e)
            products([whole(d) for d in t_dirs])
            if e == 1:
                middle_reduce(0)
        else:
            set_y(0)
            set_x_early(0)
            absorb((6,), plain(6), True)
            absorb((7,), plain(7))
            for d in (2, 3, 8):
                convert(d)
            set_x_late(0)
            absorb((4, 5), mix_x)
            set_t(0)
            absorb((0, 1), mix_t if n_ta == 2 else plain(0, 1))
            fold_early()
        for p in range(PARTS):
            set_z(e, far, 2, p)
        products([whole(2 + far, 2)])
        coeffs = None
        if e == 2:
            values = end_reduce(0, 4)
            set_gram(0, values[:1])
            set_gram(1, values[1:])
            coeffs = next_coeffs(2)
        elif e == 3:
            set_gram(2, end_reduce(1, 5))
            coeffs = next_coeffs(3)
        elif e == 4:
            set_gram(3, end_reduce(2, 7))
        for p in range(PARTS):
            set_z(e, 1 - far, 3, p)
            products([(3 - far, 3, p * width, width)])
        hop_done()
        if e < last:
            invert(e, coeffs, functools.partial(send_part, e + 1))
            send_rest(e + 1)
        else:
            invert(e, coeffs, lambda p: None)
    start_all(dots(pairs_of(ITERS)))

    for j in range(3):
        hess_column(j)
        factor_row(j)
    set_gram(4, end_reduce(3, 9))
    hess_column(3)
    factor_row(3)

    shape = hes_ref.shape[1:]
    part_at = lax.broadcasted_iota(jnp.int32, shape, 0)
    row_at = lax.broadcasted_iota(jnp.int32, shape, 1)

    def write_column(j):
        table = jnp.zeros(shape, jnp.float32)
        for i in range(j + 2):
            re, im = (x[:shape[0], :shape[1]] for x in hess[i][j])
            re = re + 1.0 if i == j else re
            table = jnp.where(row_at == i, jnp.where(part_at == 0, re, im), table)
        hes_ref[j] = table

    for j in range(last):
        write_column(j)

    for cp in pending:
        cp.wait_send()
    set_gram(5, end_all(DOTS))
    factor_row(last)
    weights = [None] * ITERS
    for j in reversed(range(ITERS)):
        total = forward[j]
        for m in range(j + 1, ITERS):
            total = csub(total, cmul_conj(low[m][j], weights[m]))
        weights[j] = cscale(total, inv_low[j])
    outer = [None] * n
    for j in range(ITERS):
        for l in range(j + 2):
            if shifted[l][j] is not None:
                outer[l] = cadd(outer[l], times(weights[j], shifted[l][j], l == j + 1))
    for k in every:
        at = pl.ds(k * SUB, SUB)
        left = (ys[0, 0, at], ys[0, 1, at])
        answer = None
        for l in range(n):
            y = (ys[l, 0, at], ys[l, 1, at])
            if l < ITERS:
                answer = cadd(answer, cmul(weights[l], y))
            left = csub(left, cmul(outer[l], y))
        for c in range(2):
            sol_ref[c, at] = answer[c]
            res_ref[c, at] = left[c]
    hess_column(last)
    write_column(last)

    others = red_all.at[pl.ds(0, n_all - 1)]
    pltpu.make_async_copy(others, others, all_send).wait()


def hand_on(*refs):
    half = len(refs) // 2
    for i in range(half):
        refs[half + i][...] = refs[i][...]


def solution(mesh):
    sizes = tuple(mesh.shape[a] for a in ("ta", "gz", "xy"))

    def per_device(source, inverse, coarse_links):
        comp, lanes = source.shape[1], source.shape[4]
        f32 = jnp.float32
        field = (2, comp, lanes)
        pitch = comp + 1
        mats = (9 * comp * pitch, lanes)
        n_two = sizes[0] * sizes[1]
        dma = pltpu.SemaphoreType.DMA
        hbm = pl.BlockSpec(memory_space=pl.ANY)
        vmem = pl.BlockSpec(memory_space=pltpu.VMEM)
        sol, res, hes = pl.pallas_call(
            functools.partial(kernel, sizes),
            out_shape=(
                pltpu.VMEM(field, f32),
                pltpu.VMEM(field, f32),
                pltpu.VMEM((ITERS, 2, ITERS + 1), f32),
            ),
            in_specs=[hbm, hbm, hbm],
            out_specs=(vmem, vmem, vmem),
            scratch_shapes=[
                pltpu.VMEM((9, 2, comp, comp, lanes), coarse_links.dtype),
                pltpu.VMEM(mats, f32),
                pltpu.VMEM(mats, f32),
                pltpu.VMEM(mats, f32),
                pltpu.VMEM((9, 3, comp, lanes), f32),
                pltpu.VMEM((3 * comp // SUB, SUB, lanes), f32),
                pltpu.VMEM((3, comp, SUB, lanes), f32),
                pltpu.VMEM((ITERS + 1, *field), f32),
                pltpu.VMEM((ITERS, 2, *field), f32),
                pltpu.VMEM((ITERS, 2, *field), f32),
                pltpu.VMEM((ITERS, 2, 2, SUB, lanes), f32),
                pltpu.VMEM((ITERS, 2, 2, SUB, lanes), f32),
                pltpu.VMEM((ITERS - 1, sizes[2], 1, lanes), f32),
                pltpu.VMEM((ITERS - 1, n_two, 1, lanes), f32),
                pltpu.VMEM((n_two * sizes[2], 1, lanes), f32),
                pltpu.VMEM((ITERS, 1, lanes), f32),
                pltpu.VMEM((ITERS - 1, 1, lanes), f32),
                dma((9,)),
                dma,
                dma((ITERS, 2)), dma((ITERS, 2)),
                dma((ITERS, 2, PARTS)), dma((ITERS, 2, PARTS)),
                dma((ITERS, 2)), dma((ITERS, 2)),
                dma((ITERS - 1, sizes[2])), dma((ITERS - 1, sizes[2])),
                dma((ITERS - 1, n_two)), dma((ITERS - 1, n_two)),
                dma, dma,
            ],
            compiler_params=pltpu.CompilerParams(
                collective_id=0, has_side_effects=True, vmem_limit_bytes=62 * 1024 * 1024),
        )(
            source.reshape(field),
            inverse.reshape(2, comp, comp, lanes),
            coarse_links.reshape(8, 2, comp, comp, lanes),
        )
        results = (sol, res, hes)
        sol, res, hes = pl.pallas_call(
            hand_on,
            out_shape=tuple(jax.ShapeDtypeStruct(x.shape, x.dtype) for x in results),
            in_specs=[vmem] * 3,
            out_specs=(vmem,) * 3,
        )(*(pltpu.with_memory_space_constraint(x, pltpu.VMEM) for x in results))
        return sol.reshape(source.shape), res.reshape(source.shape), hes.transpose(1, 2, 0)

    specs = (
        P(None, None, "ta", "gz", "xy"),
        P(None, None, None, "ta", "gz", "xy"),
        P(None, None, None, None, "ta", "gz", "xy"),
    )
    return jax.shard_map(
        per_device,
        mesh=mesh,
        in_specs=specs,
        out_specs=(specs[0], specs[0], P()),
        check_vma=False,
    )
```
